32 devices in a mesh: blk: 2 (over core), pts: 4 (over y, x), bond: 4 (over z).
Axes of the slice: x: 2, y: 2, z: 4, core: 2. Of those that a mesh axis runs over, the one named last changes fastest.
Arguments:
- mps: bfloat16 [2, 1024, 2, 1024], P('blk', None, None, 'bond'), may hold values from -1 to 2, as said below
- couplings: float32 [64, 3], replicated, may hold values from 0.5 to 2
- point_ids: int32 [4], P('pts'), may hold values from 0 to 63
- site_group: int32 [2], P('blk'), may hold values from 0 to 7
- field_levels: float32 [8], replicated, may hold values from 0.3 to 3
- left_cut: float32 [1024, 1024], P('bond'), may hold values from -200 to 200, as said below
- right_cut: float32 [1024, 1024], P('bond'), may hold values from -200 to 200, as said below
Outputs:
- left_env: bfloat16 [2, 4, 5, 1024, 1024], P('blk', 'pts', None, 'bond')
- right_env: bfloat16 [2, 4, 5, 1024, 1024], P('blk', 'pts', None, 'bond')
- energies: float32 [4], P('pts')
The draws below stay inside these ranges and needn't reach their ends.
Inputs may be any that keep to these rules, and one draw needn't show every extreme that they name: `mps`: each site tensor is the identity on spin 0 plus noise on both spins. `left_cut`: A symmetric matrix. `right_cut`: A symmetric matrix.
All inputs are finite; a program needn't handle non-finite values.
Results may differ from the reference program's by a relative error of at most 0.0066.
Values may be sent and summed in bfloat16 or wider, within the bound.
No kernel may reach another device: no remote copies, remote signals or barrier semaphores. Data moves between devices by JAX's collectives and lax.ppermute only.
A program may use at most 64 MiB of HBM per device.

```python
import math
import jax
import jax.numpy as jnp
from jax import lax

CHI = 1024
NPARAM = 64
GROUPS = 8
SITES = 2
PTS = 4


def draw_mps(key, part):
    first_key = jax.random.fold_in(jax.random.fold_in(key, 11), 0)
    noise = jax.random.truncated_normal(first_key, -4.0, 4.0, (SITES, CHI, 2, CHI), jnp.float32) / math.sqrt(CHI)
    spin_weight = jnp.array([0.3, 0.45], dtype=jnp.float32)
    spin_unit = jnp.array([1.0, 0.0], dtype=jnp.float32)
    identity = jnp.eye(CHI, dtype=jnp.float32)
    tensor = noise * spin_weight[None, None, :, None] + identity[None, :, None, :] * spin_unit[None, None, :, None]
    return tensor.astype(jnp.bfloat16)


def draw_cut(key):
    first_key = jax.random.fold_in(key, 0)
    factor = jax.random.truncated_normal(first_key, -4.0, 4.0, (CHI, CHI), jnp.float32) / math.sqrt(CHI)
    matrix = jnp.dot(factor, factor.T, precision=lax.Precision.HIGHEST) + jnp.eye(CHI, dtype=jnp.float32)
    return 0.5 * (matrix + matrix.T)


def draw_left_cut(key, part):
    return draw_cut(jax.random.fold_in(key, 21))


def draw_right_cut(key, part):
    return draw_cut(jax.random.fold_in(key, 22))


def plant(result, rng, smallest, largest):
    shape = result.shape
    place = [jax.random.randint(jax.random.fold_in(rng, axis), (), 0, shape[axis]) for axis in range(len(shape))]
    result = result.at[tuple(place)].set(smallest)
    longest = shape.index(max(shape))
    place[longest] = (place[longest] + 1) % shape[longest]
    return result.at[tuple(place)].set(largest)


def setup_inputs(seed: int = 0) -> dict:
    seeds = jax.random.split(jax.random.key(seed), 8)
    return {
        "mps": draw_mps(jax.random.fold_in(seeds[7], 71), 0),
        "couplings": jnp.clip(jax.random.uniform(seeds[1], (NPARAM, 3), jnp.float32, 0.5, 2.0), 0.5, 2.0),
        "point_ids": plant(jax.random.randint(seeds[2], (PTS,), 0, NPARAM), jax.random.fold_in(seeds[2], 1), 0, NPARAM - 1).astype(jnp.int32),
        "site_group": jax.random.randint(seeds[3], (SITES,), 0, GROUPS).astype(jnp.int32),
        "field_levels": jnp.clip(jnp.exp(jax.random.uniform(seeds[4], (GROUPS,), jnp.float32, math.log(0.3), math.log(3.0))), 0.3, 3.0),
        "left_cut": draw_left_cut(jax.random.fold_in(seeds[7], 71), 0),
        "right_cut": draw_right_cut(jax.random.fold_in(seeds[7], 71), 0),
    }


def mpo_table(coupling, field_term):
    identity = jnp.eye(2, dtype=jnp.float32)
    raising = jnp.array([[0.0, 1.0], [0.0, 0.0]], dtype=jnp.float32)
    lowering = jnp.array([[0.0, 0.0], [1.0, 0.0]], dtype=jnp.float32)
    diagonal_spin = jnp.array([[0.5, 0.0], [0.0, -0.5]], dtype=jnp.float32)
    zeros_block = jnp.zeros((2, 2), jnp.float32)
    half_xy = 0.5 * coupling[0]
    table_rows = [[identity, zeros_block, zeros_block, zeros_block, zeros_block], [raising, zeros_block, zeros_block, zeros_block, zeros_block], [lowering, zeros_block, zeros_block, zeros_block, zeros_block], [diagonal_spin, zeros_block, zeros_block, zeros_block, zeros_block], [coupling[2] * field_term * diagonal_spin, half_xy * lowering, half_xy * raising, coupling[1] * diagonal_spin, identity]]
    return jnp.stack([jnp.stack(table_row) for table_row in table_rows])

def mirrored(environment):
    return jnp.stack([environment[0], environment[2], environment[1], environment[3], environment[4]])

def advance(environment, tensor, weights):
    tensor_wide = tensor.astype(jnp.float32)
    ket_part = jnp.einsum('wyx,xsz->wsyz', mirrored(environment).astype(jnp.float32), tensor_wide, precision=lax.Precision.HIGHEST).astype(jnp.bfloat16)
    mixed_part = jnp.einsum('wsyz,wstv->vtyz', ket_part.astype(jnp.float32), weights, precision=lax.Precision.HIGHEST).astype(jnp.bfloat16)
    return jnp.einsum('vtyz,ytq->vzq', mixed_part.astype(jnp.float32), tensor_wide, precision=lax.Precision.HIGHEST)

def normalized(values):
    mean_square = jnp.mean(values * values)
    return (values * lax.rsqrt(mean_square + 1e-06)).astype(jnp.bfloat16)

def reference(mps, couplings, point_ids, site_group, field_levels, left_cut, right_cut):
    params = couplings[point_ids]
    site_fields = field_levels[site_group]
    mirror_mps = jnp.transpose(mps, (0, 3, 2, 1))
    zero_block = jnp.zeros((4, CHI, CHI), jnp.float32)
    left_start = jnp.concatenate([zero_block, left_cut[None]], 0).astype(jnp.bfloat16)
    right_start = jnp.concatenate([right_cut[None], zero_block], 0).astype(jnp.bfloat16)
    site_range = jnp.arange(SITES, dtype=jnp.int32)

    def one_point(coupling):

        def left_turn(environment, site_index):
            table = mpo_table(coupling, site_fields[site_index])
            weights = jnp.transpose(table, (0, 2, 3, 1))
            updated = normalized(advance(environment, mps[site_index], weights))
            return (updated, updated)

        def right_turn(environment, site_index):
            table = mpo_table(coupling, site_fields[site_index])
            weights = jnp.transpose(table, (1, 2, 3, 0))
            updated = normalized(advance(environment, mirror_mps[site_index], weights))
            return (updated, updated)
        _, left_list = lax.scan(left_turn, left_start, site_range)
        _, right_back = lax.scan(right_turn, right_start, site_range[::-1])
        right_list = right_back[::-1]
        meet_left = left_list[SITES // 2 - 1].astype(jnp.float32)
        meet_right = right_list[SITES // 2].astype(jnp.float32)
        numer = jnp.sum(meet_left * meet_right)
        denom = jnp.sum(meet_left[4] * meet_right[0])
        return (left_list, right_list, numer / denom / SITES)
    left_all, right_all, energies = lax.map(one_point, params)
    return (jnp.transpose(left_all, (1, 0, 2, 3, 4)), jnp.transpose(right_all, (1, 0, 2, 3, 4)), energies)
```

```python
import functools

import jax
import jax.numpy as jnp
from jax import lax
from jax.experimental import pallas as pl
from jax.experimental.pallas import tpu as pltpu
from jax.sharding import PartitionSpec as P

F32 = jnp.float32
BF16 = jnp.bfloat16
EPS = 1e-06
SHRINK = 2.0**-8


def dot_nn(lhs, rhs):
    return lax.dot_general(lhs, rhs, (((1,), (0,)), ((), ())), preferred_element_type=F32)


def dot_nt(lhs, rhs):
    return lax.dot_general(lhs, rhs, (((1,), (1,)), ((), ())), preferred_element_type=F32)


def shifted(value, axis, step):
    count = lax.axis_size(axis)
    return lax.ppermute(value, axis, [(i, (i + step) % count) for i in range(count)])


def crossed(value, axis, mask):
    count = lax.axis_size(axis)
    return lax.ppermute(value, axis, [(i, i ^ mask) for i in range(count)])


def swapped(value):
    return shifted(value, "blk", 1)


def power_of_two(count):
    return count & (count - 1) == 0


def bond_total(value):
    count = lax.axis_size("bond")
    if count == 1:
        return value
    if not power_of_two(count) or count > 8:
        return lax.psum(value, "bond")
    parts = [value] + [crossed(value, "bond", mask) for mask in range(1, count)]
    while len(parts) > 1:
        parts = [parts[i] + parts[i + 1] for i in range(0, len(parts), 2)]
    return parts[0]


def gather_pieces(tensor, cut):
    points = lax.axis_size("pts")
    shards = lax.axis_size("bond")
    chi = tensor.shape[1]
    width = tensor.shape[2]
    part = chi // points
    packs = [
        jnp.concatenate(
            [
                tensor[:, q * part : (q + 1) * part, :].reshape(2 * part, width),
                cut[:, q * part : (q + 1) * part],
            ]
        )
        for q in range(points)
    ]
    here = lax.axis_index("pts")
    mine = lax.dynamic_index_in_dim(jnp.stack(packs), here, 0, keepdims=False)
    found = []
    for step in range(1, shards):
        came = shifted(mine, "bond", step)
        found.append((came, step, 0))
        for mask in range(1, points):
            found.append((crossed(came, "pts", mask), step, mask))
    local = [(packs[q], 0, q) for q in range(points)]
    return local, found


def energy_kernel(shape, plan, scal, ints, xt_ref, *refs):
    chi, width, part, points, shards = shape
    count = len(plan)
    sources = refs[:count]
    raw, sums = refs[count : count + 2]
    own, oth, own_cut, oth_cut, xa, xb, va, t1, t2, yg, sems = refs[count + 2 :]
    core, here, spot = ints[0], ints[1], ints[2]
    tile = 256 if chi % 256 == 0 else chi
    tiles = chi // tile

    copies = []
    for index, (source, (is_other, step, mask, local)) in enumerate(zip(sources, plan)):
        site = oth if is_other else own
        site_cut = oth_cut if is_other else own_cut
        if step is None:
            copies.append((source, site if mask == 0 else site_cut))
            continue
        shard = lax.rem(spot + shards - step, shards)
        quarter = mask if local else lax.bitwise_xor(here, mask)
        rows = pl.ds(pl.multiple_of(quarter * part, part), part)
        cols = pl.ds(pl.multiple_of(shard * width, width), width)
        copies.append((source.at[pl.ds(0, part)], site.at[0, rows, cols]))
        copies.append((source.at[pl.ds(part, part)], site.at[1, rows, cols]))
        cut_rows = pl.ds(pl.multiple_of(shard * width, width), width)
        cut_cols = pl.ds(pl.multiple_of(quarter * part, part), part)
        copies.append((source.at[pl.ds(2 * part, width)], site_cut.at[cut_rows, cut_cols]))
    started = []
    for index, (source, target) in enumerate(copies):
        copy = pltpu.make_async_copy(source, target, sems.at[index])
        copy.start()
        started.append(copy)
    for copy in started:
        copy.wait()

    mine = pl.ds(pl.multiple_of(spot * width, width), width)

    def run(first, last, xs_first_transposed):
        def cols_of(ref, index, form, at):
            return ref[index, :, at] if form is dot_nn else ref[index, at, :]

        x_first, x_second = xa, xb
        for s in range(2):
            rows = pl.ds(s * width, width)
            if xs_first_transposed:
                x_first[rows, :] = xt_ref[s]
                x_second[rows, :] = own[s, mine, :]
            else:
                x_first[rows, :] = own[s, mine, :]
                x_second[rows, :] = xt_ref[s]

        def cut_first(j, carry):
            at = pl.ds(pl.multiple_of(j * tile, tile), tile)
            va[:, at] = dot_nn(x_first[...], own_cut[:, at]).astype(BF16)
            return carry

        lax.fori_loop(0, tiles, cut_first, 0)

        def stage_one(j, carry):
            at = pl.ds(pl.multiple_of(j * tile, tile), tile)
            up = first(va[...], cols_of(own, 0, first, at))
            down = first(va[...], cols_of(own, 1, first, at))
            p00, p10 = up[:width], up[width:]
            p01, p11 = down[:width], down[width:]
            plus, minus = p00 + p11, p00 - p11
            raw[0, :, at] = plus
            raw[1, :, at] = minus
            raw[2, :, at] = p01
            raw[3, :, at] = p10
            return tuple(c + jnp.sum(v * v) for c, v in zip(carry, (plus, minus, p01, p10)))

        zero = jnp.zeros((), F32)
        s_plus, s_minus, s_01, s_10 = lax.fori_loop(0, tiles, stage_one, (zero,) * 4)
        sums[0] = s_plus
        sums[1] = s_minus
        sums[2] = s_01 + s_10

        def first_product(j, carry):
            at = pl.ds(pl.multiple_of(j * tile, tile), tile)
            for t in range(2):
                rows = pl.ds(t * 2 * width, 2 * width)
                t1[rows, at] = first(x_second[...], cols_of(oth, t, first, at)).astype(BF16)
            return carry

        lax.fori_loop(0, tiles, first_product, 0)

        def cut_second(j, carry):
            at = pl.ds(pl.multiple_of(j * tile, tile), tile)
            t2[:, at] = dot_nn(t1[...], oth_cut[:, at]).astype(BF16)
            return carry

        lax.fori_loop(0, tiles, cut_second, 0)

        plus_scale, minus_scale, xy_scale, field_scale = scal[0], scal[1], scal[2], scal[3]

        def mixing(j, carry):
            at = pl.ds(pl.multiple_of(j * tile, tile), tile)
            q0 = last(t2[: 3 * width], cols_of(oth, 0, last, at))
            q1 = last(t2[width:], cols_of(oth, 1, last, at))
            a0, a1, a01 = q0[:width], q0[width : 2 * width], q0[2 * width :]
            b10, b0, b1 = q1[:width], q1[width : 2 * width], q1[2 * width :]
            sum0, sum1 = a0 + b0, a1 + b1
            y0 = plus_scale * (a0 - b0) + xy_scale * b10 + field_scale * sum0
            y1 = minus_scale * (a1 - b1) + xy_scale * a01 - field_scale * sum1
            yg[pl.ds(0, width), at] = y0.astype(BF16)
            yg[pl.ds(width, width), at] = sum0.astype(BF16)
            yg[pl.ds(2 * width, width), at] = sum1.astype(BF16)
            yg[pl.ds(3 * width, width), at] = y1.astype(BF16)
            return carry

        lax.fori_loop(0, tiles, mixing, 0)

        def stage_two(j, carry):
            at = pl.ds(pl.multiple_of(j * tile, tile), tile)
            r0 = last(yg[: 3 * width], cols_of(own, 0, last, at))
            r1 = last(yg[width:], cols_of(own, 1, last, at))
            special = r0[:width] + r1[2 * width :]
            p00, p10 = r0[width : 2 * width], r0[2 * width :]
            p01, p11 = r1[:width], r1[width : 2 * width]
            plus, minus = p00 + p11, p00 - p11
            raw[4, :, at] = plus
            raw[5, :, at] = minus
            raw[6, :, at] = p01
            raw[7, :, at] = p10
            raw[8, :, at] = special
            edge = own_cut[mine, at].astype(F32)
            squares = tuple(
                c + jnp.sum(v * v) for c, v in zip(carry, (plus, minus, p01, p10, special))
            )
            return squares + (
                carry[5] + jnp.sum(special * edge),
                carry[6] + jnp.sum(plus * edge),
            )

        s_plus, s_minus, s_01, s_10, s_special, numer, denom = lax.fori_loop(
            0, tiles, stage_two, (zero,) * 7
        )
        sums[3] = s_plus
        sums[4] = s_minus
        sums[5] = s_01 + s_10
        sums[6] = s_special
        sums[7] = numer
        sums[8] = denom

    @pl.when(core == 0)
    def _():
        run(dot_nn, dot_nt, True)

    @pl.when(core != 0)
    def _():
        run(dot_nt, dot_nn, False)


def finish_kernel(scal, ints, raw, left, right):
    def one(out, base, order):
        for v, (index, coef) in enumerate(order):
            out[0, 0, v] = (raw[index] * scal[coef]).astype(BF16)

    @pl.when(ints[0] == 0)
    def _():
        one(left, 0, ((1, 0), (3, 1), (2, 1), (1, 2), (0, 3)))
        one(right, 0, ((4, 4), (6, 5), (7, 5), (5, 6), (8, 4)))

    @pl.when(ints[0] != 0)
    def _():
        one(left, 0, ((8, 4), (7, 5), (6, 5), (5, 6), (4, 4)))
        one(right, 0, ((0, 3), (2, 1), (3, 1), (1, 2), (1, 0)))


def body(mps, couplings, point_ids, site_group, field_levels, left_cut, right_cut):
    blocks = lax.axis_size("blk")
    points = lax.axis_size("pts")
    shards = lax.axis_size("bond")
    core = lax.axis_index("blk")
    here = lax.axis_index("pts")
    spot = lax.axis_index("bond")
    chi, width = mps.shape[1], mps.shape[3]
    part = chi // points
    rows, entries = width, 5 * chi * chi

    param_count = couplings.shape[0]
    chosen = (point_ids[0] == jnp.arange(param_count, dtype=jnp.int32)).astype(F32)
    params = jnp.sum(chosen[:, None] * couplings, axis=0)
    group_count = field_levels.shape[0]
    level = jnp.sum(
        jnp.where(site_group[0] == jnp.arange(group_count, dtype=jnp.int32), field_levels, 0.0)
    )
    level_other = swapped(jnp.broadcast_to(level, (8, 128)))[0, 0]
    half_xy, coupling_z, field = 0.5 * params[0], params[1], params[2]
    field_own, field_other = field * level, field * level_other

    tensor = jnp.transpose(mps[0], (1, 0, 2))
    flipped = jnp.transpose(mps[0], (1, 2, 0))
    cut = (jnp.where(core == 0, left_cut, right_cut) * SHRINK).astype(BF16)

    if points == 4 and shards == 4 and part == width:
        local, found = gather_pieces(tensor, cut)
        sources, plan = [], []
        for pieces, is_local in ((local, True), (found, False)):
            for piece, step, mask in pieces:
                sources.append(piece)
                plan.append((False, step, mask, is_local))
                sources.append(swapped(piece))
                plan.append((True, step, mask, is_local))
    else:
        full = lax.all_gather(tensor, "bond", axis=2, tiled=True)
        full_cut = lax.all_gather(cut, "bond", axis=0, tiled=True)
        sources = [full, full_cut, swapped(full), swapped(full_cut)]
        plan = [(False, None, 0, True), (False, None, 1, True), (True, None, 0, True), (True, None, 1, True)]

    ints = jnp.stack([core, here, spot]).astype(jnp.int32)
    scal = jnp.stack(
        [
            0.5 * field_other + 0.25 * coupling_z,
            0.5 * field_other - 0.25 * coupling_z,
            half_xy,
            0.5 * field_own,
        ]
    )
    smem = pl.BlockSpec(memory_space=pltpu.SMEM)
    vmem = pl.BlockSpec(memory_space=pltpu.VMEM)
    hbm = pl.BlockSpec(memory_space=pl.ANY)
    raw, sums = pl.pallas_call(
        functools.partial(energy_kernel, (chi, width, part, points, shards), tuple(plan)),
        out_shape=(
            jax.ShapeDtypeStruct((9, rows, chi), F32),
            jax.ShapeDtypeStruct((16,), F32),
        ),
        in_specs=[smem, smem, vmem] + [hbm] * len(sources),
        out_specs=(vmem, smem),
        scratch_shapes=[
            pltpu.VMEM((2, chi, chi), BF16),
            pltpu.VMEM((2, chi, chi), BF16),
            pltpu.VMEM((chi, chi), BF16),
            pltpu.VMEM((chi, chi), BF16),
            pltpu.VMEM((2 * rows, chi), BF16),
            pltpu.VMEM((2 * rows, chi), BF16),
            pltpu.VMEM((2 * rows, chi), BF16),
            pltpu.VMEM((4 * rows, chi), BF16),
            pltpu.VMEM((4 * rows, chi), BF16),
            pltpu.VMEM((4 * rows, chi), BF16),
            pltpu.SemaphoreType.DMA((3 * len(sources),)),
        ],
        compiler_params=pltpu.CompilerParams(vmem_limit_bytes=56 * 1024 * 1024),
        cost_estimate=pl.CostEstimate(
            flops=52 * rows * chi * chi, bytes_accessed=20 * chi * chi, transcendentals=0
        ),
        name="environments",
    )(scal, ints, flipped, *sources)

    one = jnp.ones((), F32)
    is_left = core == 0
    first_field = 0.5 * field_own
    xy_left, z_left = half_xy, 0.5 * coupling_z
    xy_first = jnp.where(is_left, xy_left, one)
    z_first = jnp.where(is_left, z_left, 0.5 * one)
    xy_second = jnp.where(is_left, one, xy_left)
    z_second = jnp.where(is_left, 0.5 * one, z_left)
    square_first = (
        sums[0] + (first_field**2 + z_first**2) * sums[1] + xy_first**2 * sums[2]
    )
    square_second = sums[3] + z_second**2 * sums[4] + xy_second**2 * sums[5] + sums[6]
    packed = jnp.stack([square_first, square_second, sums[7], sums[8]])
    packed = jnp.broadcast_to(jnp.pad(packed, (0, 4))[:, None], (8, 128))
    totals = bond_total(packed)
    across = swapped(totals)
    regrow = 1.0 / SHRINK

    def first_scale(total):
        return regrow * lax.rsqrt(total * (regrow * regrow) / entries + EPS)

    scale_one = first_scale(totals[0, 0])
    scale_mid = first_scale(across[0, 0])
    scale_two = scale_mid * lax.rsqrt(scale_mid * scale_mid * (totals[1, 0] / entries) + EPS)
    energy = jnp.where(is_left, across[2, 0] / across[3, 0], totals[2, 0] / totals[3, 0]) / blocks

    finals = jnp.stack(
        [
            scale_one * first_field,
            scale_one * xy_first,
            scale_one * z_first,
            scale_one,
            scale_two,
            scale_two * xy_second,
            scale_two * z_second,
        ]
    )
    band = min(rows, 64)
    out = jax.ShapeDtypeStruct((1, 1, 5, rows, chi), BF16)
    out_spec = pl.BlockSpec((1, 1, 5, band, chi), lambda i: (0, 0, 0, i, 0))
    left_env, right_env = pl.pallas_call(
        finish_kernel,
        grid=(rows // band,),
        out_shape=(out, out),
        in_specs=[smem, smem, pl.BlockSpec((9, band, chi), lambda i: (0, i, 0))],
        out_specs=(out_spec, out_spec),
        name="finish",
    )(finals, ints, raw)
    return left_env, right_env, energy[None]


def solution(mesh):
    placed = (
        P("blk", None, None, "bond"),
        P(),
        P("pts"),
        P("blk"),
        P(),
        P("bond", None),
        P("bond", None),
    )
    return jax.shard_map(
        body,
        mesh=mesh,
        in_specs=placed,
        out_specs=(
            P("blk", "pts", None, "bond", None),
            P("blk", "pts", None, "bond", None),
            P("pts"),
        ),
        check_vma=False,
    )
```

```python
import functools

import jax
import jax.numpy as jnp
from jax import lax
from jax.experimental import pallas as pl
from jax.experimental.pallas import tpu as pltpu
from jax.sharding import PartitionSpec as P


F32 = jnp.float32
BF16 = jnp.bfloat16
EPS = 1e-06
SHRINK = 2.0**-8


def dot_nn(lhs, rhs):
    return lax.dot_general(lhs, rhs, (((1,), (0,)), ((), ())), preferred_element_type=F32)


def dot_nt(lhs, rhs):
    return lax.dot_general(lhs, rhs, (((1,), (1,)), ((), ())), preferred_element_type=F32)


def crossed(value, axis, mask):
    count = lax.axis_size(axis)
    return lax.ppermute(value, axis, [(i, i ^ mask) for i in range(count)])


def swapped(value):
    count = lax.axis_size("blk")
    return lax.ppermute(value, "blk", [(i, (i + 1) % count) for i in range(count)])


def power_of_two(count):
    return count & (count - 1) == 0


SIDES = ((0, 1), (1, 0), (2, 3), (3, 2))
CENTRE = ((1, 2), (2, 1))
OUTWARD = ((1, 0), (2, 3))
INWARD = ((0, 1), (3, 2))


def gathered(mps, cut):
    points = lax.axis_size("pts")
    chi, width = mps.shape[0], mps.shape[2]
    part = chi // points
    here, spot = lax.axis_index("pts"), lax.axis_index("bond")
    quarter = lax.dynamic_slice(mps, (here * part, 0, 0), (part, 2, width))
    mine = jnp.concatenate([quarter[:, 0], quarter[:, 1]])
    near = lax.ppermute(mine, "bond", SIDES)
    centre = lax.ppermute(mine, "bond", CENTRE)
    inner = lax.ppermute(near, "bond", CENTRE)
    outer = lax.ppermute(centre, "bond", OUTWARD)
    ends = lax.ppermute(inner, "bond", OUTWARD)
    end = (spot == 0) | (spot == 3)
    middle = jnp.where(end, outer, centre)
    ends, _ = lax.optimization_barrier((ends, middle))
    groups = (near, middle, jnp.where(end, ends, inner))
    pieces = []
    for index, column in enumerate(groups):
        along_x = crossed(column, "pts", 1)
        along_y = crossed(column, "pts", 2)
        if index % 2 == 0:
            across = crossed(along_y, "pts", 1)
        else:
            across = crossed(along_x, "pts", 2)
        pieces += [column, along_x, along_y, across]

    def block(step):
        return lax.dynamic_slice(cut, (0, step * part), (width, part))

    pair_side = jnp.concatenate([block(jnp.where(spot < 2, 2, 1)), block(spot)])
    pair_centre = jnp.concatenate([block(lax.bitwise_xor(spot, 1)), block(spot)])
    far = block(3 - spot)
    pair_side = lax.ppermute(pair_side, "bond", SIDES)
    pair_centre = lax.ppermute(pair_centre, "bond", CENTRE)
    pair_inner = lax.ppermute(pair_side, "bond", CENTRE)
    pair_outer = lax.ppermute(pair_centre, "bond", OUTWARD)
    pair_ends = lax.ppermute(pair_inner, "bond", OUTWARD)
    far = lax.ppermute(far, "bond", INWARD)
    return pieces, [pair_side, pair_centre, pair_inner, pair_outer, pair_ends, far]


MIRRORED = tuple(
    sum((4 * i + j) << (4 * t) for t, (i, j) in enumerate(pairs))
    for pairs in (
        ((0, 1), (0, 2), (0, 3), (1, 2), (2, 3), (3, 1)),
        ((1, 0), (1, 2), (1, 3), (0, 2), (2, 3), (0, 3)),
        ((2, 0), (2, 1), (2, 3), (3, 1), (1, 0), (3, 0)),
        ((3, 0), (3, 1), (3, 2), (2, 1), (1, 0), (0, 2)),
    )
)


def shard_of(group, spot):
    table = ((1, 0, 3, 2), (2, 2, 1, 1), (3, 3, 0, 0))[group]
    shard = jnp.int32(table[0])
    for index in range(1, 4):
        shard = jnp.where(spot == index, table[index], shard)
    return shard


def point_scalars(couplings, point, group, group_other, levels):
    half_xy = 0.5 * couplings[0, point[0]]
    coupling_z = couplings[1, point[0]]
    field = couplings[2, point[0]]
    return half_xy, coupling_z, field * levels[group[0]], field * levels[group_other[0]]


def spread(rows):
    at = lax.broadcasted_iota(jnp.int32, (8, 128), 0)
    out = jnp.zeros((8, 128), F32)
    for index, value in enumerate(rows):
        out = jnp.where(at == index, value, out)
    return out


class Copies:
    def __init__(self, sems):
        self.sems, self.count, self.lists = sems, 0, {}

    def start(self, name, source, target, when=None):
        copy = pltpu.make_async_copy(source, target, self.sems.at[self.count])
        self.count += 1
        self.lists.setdefault(name, []).append((copy, when))
        if when is None:
            copy.start()
        else:
            pl.when(when)(copy.start)

    def wait(self, name):
        for copy, when in self.lists.get(name, ()):
            if when is None:
                copy.wait()
            else:
                pl.when(when)(copy.wait)


def fill_site(copies, name, sources, shape, site):
    _, width, part, _, _ = shape
    here, spot = lax.axis_index("pts"), lax.axis_index("bond")
    mine = pl.ds(pl.multiple_of(spot * width, width), width)
    copies.start(name, sources[0].at[0], site.at[0, :, mine])
    copies.start(name, sources[0].at[1], site.at[1, :, mine])
    for group in range(3):
        cols = pl.ds(pl.multiple_of(shard_of(group, spot) * width, width), width)
        for slot in range(4):
            piece = sources[1 + 4 * group + slot]
            rows = pl.ds(pl.multiple_of(lax.bitwise_xor(here, slot) * part, part), part)
            copies.start(name, piece.at[pl.ds(0, part)], site.at[0, rows, cols])
            copies.start(name, piece.at[pl.ds(part, part)], site.at[1, rows, cols])


def fill_cut(copies, name, rows_here, sources, shape, site_cut):
    width = shape[1]
    spot = lax.axis_index("bond")

    def at(step):
        return pl.ds(pl.multiple_of(lax.rem(step, 4) * width, width), width)

    def block(source, index, i, j, when=None):
        copies.start(name, source.at[pl.ds(index * width, width)], site_cut.at[at(i), at(j)], when)

    mine = pl.ds(pl.multiple_of(spot * width, width), width)
    copies.start(name, rows_here, site_cut.at[mine, :])
    pair_side, pair_centre, pair_inner, pair_outer, pair_ends, far = sources
    beside, across, beyond = lax.bitwise_xor(spot, 1), 3 - spot, lax.bitwise_xor(spot, 2)
    end = (spot == 0) | (spot == 3)
    centre = (spot == 1) | (spot == 2)
    block(pair_side, 0, beside, jnp.where(spot < 2, 2, 1))
    block(pair_side, 1, beside, beside)
    block(pair_centre, 0, across, lax.bitwise_xor(across, 1), centre)
    block(pair_centre, 1, across, across, centre)
    block(pair_inner, 1, beyond, beyond, centre)
    block(pair_outer, 0, beyond, lax.bitwise_xor(beyond, 1), end)
    block(pair_outer, 1, beyond, beyond, end)
    block(pair_ends, 0, across, jnp.where(across < 2, 2, 1), end)
    block(pair_ends, 1, across, across, end)
    block(far, 0, beside, 3 - beside, centre)


def mirror_cut(shape, site_cut):
    width = shape[1]
    spot = lax.axis_index("bond")
    code = jnp.int32(MIRRORED[0])
    for index in range(1, 4):
        code = jnp.where(spot == index, MIRRORED[index], code)

    def one(t, carry):
        pair = lax.bitwise_and(lax.shift_right_logical(code, 4 * t), 15)
        i = pl.ds(pl.multiple_of(lax.shift_right_logical(pair, 2) * width, width), width)
        j = pl.ds(pl.multiple_of(lax.bitwise_and(pair, 3) * width, width), width)
        site_cut[j, i] = site_cut[i, j].T
        return carry

    lax.fori_loop(0, 6, one, 0)


def wait_all(started):
    for copy in started:
        copy.wait()


def columns_of(ref, index, form, at):
    return ref[index, :, at] if form is dot_nn else ref[index, at, :]


def tiled(chi):
    tile = 1024 if chi % 1024 == 0 else chi
    return tile, chi // tile


def facts_kernel(couplings, point, group, group_other, levels, facts):
    facts[...] = spread(point_scalars(couplings, point, group, group_other, levels))


def cut_kernel(shape, couplings, point, group, group_other, levels, rows_here, *refs):
    sources, (whole, facts, sems) = refs[:-3], refs[-3:]
    copies = Copies(sems)
    fill_cut(copies, "cut", rows_here, sources, shape, whole)
    facts_kernel(couplings, point, group, group_other, levels, facts)
    copies.wait("cut")
    mirror_cut(shape, whole)


def fact(facts, row):
    return facts[row : row + 1, 0:1]


def first_kernel(shape, grouped, facts, flipped, cut, *refs):
    chi, width = shape[:2]
    count = len(refs) - 7
    slabs, (raw, sums, xb, site, xs, va, sems) = refs[:count], refs[count:]
    core, spot = lax.axis_index("blk"), lax.axis_index("bond")
    copies = Copies(sems)
    if grouped:
        fill_site(copies, "site", slabs, shape, site)
    else:
        copies.start("site", slabs[0], site)
    half_xy, coupling_z, field_own = fact(facts, 0), fact(facts, 1), fact(facts, 2)
    tile, tiles = tiled(chi)
    mine = pl.ds(pl.multiple_of(spot * width, width), width)

    def run(form, flip, xy, z):
        def natural(ref):
            copies.wait("site")
            for s in range(2):
                ref[pl.ds(s * width, width), :] = site[s, mine, :]

        copies.lists.pop("turned", None)
        for s in range(2):
            target = (xs if flip else xb).at[pl.ds(s * width, width)]
            copies.start("turned", flipped.at[s], target)
        if flip:
            copies.wait("turned")
        else:
            natural(xs)

        def with_cut(j, carry):
            at = pl.ds(pl.multiple_of(j * tile, tile), tile)
            va[:, at] = dot_nn(xs[...], cut[:, at]).astype(BF16)
            return carry

        lax.fori_loop(0, tiles, with_cut, 0)
        if flip:
            natural(xb)
        else:
            copies.wait("turned")

        def products(j, carry):
            at = pl.ds(pl.multiple_of(j * tile, tile), tile)
            up = form(va[...], columns_of(site, 0, form, at))
            down = form(va[...], columns_of(site, 1, form, at))
            p00, p10 = up[:width], up[width:]
            p01, p11 = down[:width], down[width:]
            plus, minus = p00 + p11, p00 - p11
            raw[0, :, at] = plus.astype(BF16)
            raw[1, :, at] = minus.astype(BF16)
            raw[2, :, at] = p01.astype(BF16)
            raw[3, :, at] = p10.astype(BF16)
            squares = (plus * plus, minus * minus, p01 * p01 + p10 * p10)
            return tuple(c + jnp.sum(v) for c, v in zip(carry, squares))

        zero = jnp.zeros((), F32)
        plus, minus, xys = lax.fori_loop(0, tiles, products, (zero,) * 3)
        first_field = 0.5 * field_own
        square = plus + (first_field * first_field + z * z) * minus + xy * xy * xys
        at = lax.broadcasted_iota(jnp.int32, (8, 128), 0)
        sums[...] = jnp.where(at == (3 if flip else 4), square, 0.0)

    @pl.when(core == 0)
    def _():
        run(dot_nn, True, half_xy, 0.5 * coupling_z)

    @pl.when(core != 0)
    def _():
        run(dot_nt, False, 1.0, 0.5)


def second_kernel(shape, grouped, facts, xs, cut, far_cut, *refs):
    chi, width = shape[:2]
    count = len(refs) - 10
    slabs = refs[:count]
    raw, sums, own, oth, oth_cut, edge, t1, t2, yg, sems = refs[count:]
    core = lax.axis_index("blk")
    tile, tiles = tiled(chi)
    copies = Copies(sems)
    if grouped:
        fill_site(copies, "other", slabs[13:], shape, oth)
    else:
        copies.start("other", slabs[1], oth)
    copies.start("cut", far_cut, oth_cut)
    copies.start("own", cut, edge)
    if grouped:
        fill_site(copies, "own", slabs[:13], shape, own)
    else:
        copies.start("own", slabs[0], own)
    half_xy, coupling_z = fact(facts, 0), fact(facts, 1)
    field_own, field_other = fact(facts, 2), fact(facts, 3)
    plus_scale = 0.5 * field_other + 0.25 * coupling_z
    minus_scale = 0.5 * field_other - 0.25 * coupling_z
    field_scale = 0.5 * field_own
    copies.wait("other")

    def run(first, last, xy, z):
        def first_product(j, carry):
            at = pl.ds(pl.multiple_of(j * tile, tile), tile)
            for t in range(2):
                rows = pl.ds(t * 2 * width, 2 * width)
                t1[rows, at] = first(xs[...], columns_of(oth, t, first, at)).astype(BF16)
            return carry

        lax.fori_loop(0, tiles, first_product, 0)
        copies.wait("cut")

        def with_cut(j, carry):
            at = pl.ds(pl.multiple_of(j * tile, tile), tile)
            t2[:, at] = dot_nn(t1[...], oth_cut[:, at]).astype(BF16)
            return carry

        lax.fori_loop(0, tiles, with_cut, 0)

        def mixing(j, carry):
            at = pl.ds(pl.multiple_of(j * tile, tile), tile)
            q0 = last(t2[: 3 * width], columns_of(oth, 0, last, at))
            q1 = last(t2[width:], columns_of(oth, 1, last, at))
            a0, a1, a01 = q0[:width], q0[width : 2 * width], q0[2 * width :]
            b10, b0, b1 = q1[:width], q1[width : 2 * width], q1[2 * width :]
            sum0, sum1 = a0 + b0, a1 + b1
            y0 = plus_scale * (a0 - b0) + half_xy * b10 + field_scale * sum0
            y1 = minus_scale * (a1 - b1) + half_xy * a01 - field_scale * sum1
            yg[pl.ds(0, width), at] = y0.astype(BF16)
            yg[pl.ds(width, width), at] = sum0.astype(BF16)
            yg[pl.ds(2 * width, width), at] = sum1.astype(BF16)
            yg[pl.ds(3 * width, width), at] = y1.astype(BF16)
            return carry

        lax.fori_loop(0, tiles, mixing, 0)
        copies.wait("own")

        def products(j, carry):
            at = pl.ds(pl.multiple_of(j * tile, tile), tile)
            r0 = last(yg[: 3 * width], columns_of(own, 0, last, at))
            r1 = last(yg[width:], columns_of(own, 1, last, at))
            special = r0[:width] + r1[2 * width :]
            p00, p10 = r0[width : 2 * width], r0[2 * width :]
            p01, p11 = r1[:width], r1[width : 2 * width]
            plus, minus = p00 + p11, p00 - p11
            raw[0, :, at] = plus.astype(BF16)
            raw[1, :, at] = minus.astype(BF16)
            raw[2, :, at] = p01.astype(BF16)
            raw[3, :, at] = p10.astype(BF16)
            raw[4, :, at] = special.astype(BF16)
            border = edge[:, at].astype(F32)
            parts = (
                plus * plus + special * special,
                minus * minus,
                p01 * p01 + p10 * p10,
                special * border,
                plus * border,
            )
            return tuple(c + jnp.sum(v) for c, v in zip(carry, parts))

        zero = jnp.zeros((), F32)
        square, minus, xys, numer, denom = lax.fori_loop(0, tiles, products, (zero,) * 5)
        total = square + z * z * minus + xy * xy * xys
        sums[...] = spread([jnp.broadcast_to(total, (8, 128)), numer, denom])

    @pl.when(core == 0)
    def _():
        run(dot_nn, dot_nt, 1.0, 0.5)

    @pl.when(core != 0)
    def _():
        run(dot_nt, dot_nn, half_xy, 0.5 * coupling_z)


def first_scale(total, entries):
    regrow = 1.0 / SHRINK
    return regrow * lax.rsqrt(total * (regrow * regrow) / entries + EPS)


def summed(refs):
    parts = [ref[...] for ref in refs]
    while len(parts) > 1:
        parts = [parts[i] + parts[i + 1] for i in range(0, len(parts), 2)]
    return parts[0]


def finish_kernel(entries, facts, first, second, *refs):
    left, right, stage, sems = refs[-4:]
    core = lax.axis_index("blk")
    half_xy, coupling_z, field_own = fact(facts, 0), fact(facts, 1), fact(facts, 2)
    total = summed(refs[:-4])

    def run(row_one, row_mid, out_one, out_two, order_one, order_two):
        plain_one = first_scale(total[row_one : row_one + 1, 0:1], entries)
        middle = first_scale(total[row_mid : row_mid + 1, 0:1], entries)
        mean = total[0:1, 0:1] / entries
        plain_two = middle * lax.rsqrt(middle * middle * mean + EPS)
        started = []
        for part, (raw, out, plain, order) in enumerate(
            ((first, out_one, plain_one, order_one), (second, out_two, plain_two, order_two))
        ):
            for v, (index, weight) in enumerate(order):
                scale = plain if weight is None else plain * weight
                stage[part, v] = (raw[index].astype(F32) * scale).astype(BF16)
                copy = pltpu.make_async_copy(
                    stage.at[part, v], out.at[0, 0, v], sems.at[5 * part + v]
                )
                copy.start()
                started.append(copy)
        wait_all(started)

    xy, z, field = half_xy, 0.5 * coupling_z, 0.5 * field_own

    @pl.when(core == 0)
    def _():
        order_one = ((1, field), (3, xy), (2, xy), (1, z), (0, None))
        order_two = ((0, None), (2, None), (3, None), (1, 0.5), (4, None))
        run(3, 4, left, right, order_one, order_two)

    @pl.when(core != 0)
    def _():
        order_one = ((0, None), (2, None), (3, None), (1, 0.5), (1, field))
        order_two = ((4, None), (3, xy), (2, xy), (1, z), (0, None))
        run(4, 3, right, left, order_one, order_two)


def bond_parts(value):
    count = lax.axis_size("bond")
    if not power_of_two(count) or count > 8:
        return [lax.psum(value, "bond")]
    return [value] + [crossed(value, "bond", mask) for mask in range(1, count)]


def total_of(parts):
    parts = list(parts)
    while len(parts) > 1:
        parts = [parts[i] + parts[i + 1] for i in range(0, len(parts), 2)]
    return parts[0]


def body(mps, couplings, point_ids, site_group, field_levels, left_cut, right_cut):
    blocks = lax.axis_size("blk")
    points = lax.axis_size("pts")
    shards = lax.axis_size("bond")
    core = lax.axis_index("blk")
    chi, width = mps.shape[1], mps.shape[3]
    part = chi // points
    entries = 5 * chi * chi

    tensor = jnp.transpose(mps[0], (1, 0, 2))
    flipped = jnp.transpose(mps[0], (1, 2, 0))
    group_other = swapped(site_group)

    cut = (jnp.where(core == 0, left_cut, right_cut) * SHRINK).astype(BF16)

    shape = (chi, width, part, points, shards)
    smem = pl.BlockSpec(memory_space=pltpu.SMEM)
    vmem = pl.BlockSpec(memory_space=pltpu.VMEM)
    hbm = pl.BlockSpec(memory_space=pl.ANY)
    far = pl.BlockSpec(memory_space=pltpu.HBM)
    scalars = (couplings.T, point_ids, site_group, group_other, field_levels)
    flags = jax.ShapeDtypeStruct((8, 128), F32)
    site_scratch = [pltpu.VMEM((2, chi, chi), BF16)]
    grouped = points == 4 and shards == 4 and part == width
    if grouped:
        pieces, blocks_of_cut = gathered(mps[0], cut)
        tensors = [tensor] + pieces
        whole_cut, facts = pl.pallas_call(
            functools.partial(cut_kernel, shape),
            out_shape=(jax.ShapeDtypeStruct((chi, chi), BF16), flags),
            in_specs=[smem] * 5 + [hbm] * (1 + len(blocks_of_cut)),
            out_specs=(vmem, vmem),
            scratch_shapes=[pltpu.SemaphoreType.DMA((12,))],
            compiler_params=pltpu.CompilerParams(vmem_limit_bytes=6 * 1024 * 1024),
            cost_estimate=pl.CostEstimate(
                flops=2 * width * chi * chi, bytes_accessed=4 * chi * chi, transcendentals=0
            ),
            name="whole_cut",
        )(*scalars, cut, *blocks_of_cut)
    else:
        tensors = [lax.all_gather(tensor, "bond", axis=2, tiled=True)]
        whole_cut = lax.all_gather(cut, "bond", axis=0, tiled=True)
        facts = pl.pallas_call(
            facts_kernel, out_shape=flags, in_specs=[smem] * 5, out_specs=vmem, name="facts"
        )(*scalars)
    far_tensors = [swapped(value) for value in tensors]
    far_cut = swapped(whole_cut)

    def cost(units):
        return pl.CostEstimate(
            flops=2 * units * width * chi * chi, bytes_accessed=12 * chi * chi, transcendentals=0
        )

    doubled = jax.ShapeDtypeStruct((2 * width, chi), BF16)
    raw_one, sums_one, held_rows = pl.pallas_call(
        functools.partial(first_kernel, shape, grouped),
        out_shape=(jax.ShapeDtypeStruct((4, width, chi), BF16), flags, doubled),
        in_specs=[vmem, hbm, vmem] + [hbm] * len(tensors),
        out_specs=(vmem,) * 3,
        scratch_shapes=site_scratch
        + [pltpu.VMEM((2 * width, chi), BF16)] * 2
        + [pltpu.SemaphoreType.DMA((30,))],
        compiler_params=pltpu.CompilerParams(vmem_limit_bytes=20 * 1024 * 1024),
        cost_estimate=cost(6),
        name="first_site",
    )(facts, flipped, whole_cut, *tensors)
    sums_far = swapped(sums_one)

    raw_two, sums_two = pl.pallas_call(
        functools.partial(second_kernel, shape, grouped),
        out_shape=(jax.ShapeDtypeStruct((5, width, chi), BF16), flags),
        in_specs=[vmem, vmem] + [hbm] * (2 + 2 * len(tensors)),
        out_specs=(vmem, vmem),
        scratch_shapes=site_scratch * 2
        + [pltpu.VMEM((chi, chi), BF16)]
        + [pltpu.VMEM((width, chi), BF16)]
        + [pltpu.VMEM((4 * width, chi), BF16)] * 3
        + [pltpu.SemaphoreType.DMA((54,))],
        compiler_params=pltpu.CompilerParams(vmem_limit_bytes=32 * 1024 * 1024),
        cost_estimate=cost(20),
        name="second_site",
    )(facts, held_rows, cut, far_cut, *tensors, *far_tensors)

    parts = bond_parts(sums_two + sums_one + sums_far)
    total = total_of(parts)
    across = swapped(total)
    out = jax.ShapeDtypeStruct((1, 1, 5, width, chi), BF16)
    left, right = pl.pallas_call(
        functools.partial(finish_kernel, entries),
        out_shape=(out, out),
        in_specs=[vmem] * (3 + len(parts)),
        out_specs=(hbm, hbm),
        scratch_shapes=[
            pltpu.VMEM((2, 5, width, chi), BF16),
            pltpu.SemaphoreType.DMA((10,)),
        ],
        compiler_params=pltpu.CompilerParams(vmem_limit_bytes=20 * 1024 * 1024),
        cost_estimate=cost(6),
        name="finish",
    )(facts, raw_one, raw_two, *parts)

    total = jnp.where(core == 0, across, total)
    energies = total[1, :1] / total[2, :1] / blocks
    return left, right, energies


def solution(mesh):
    placed = (
        P("blk", None, None, "bond"),
        P(),
        P("pts"),
        P("blk"),
        P(),
        P("bond", None),
        P("bond", None),
    )

    return jax.shard_map(
        body,
        mesh=mesh,
        in_specs=placed,
        out_specs=(
            P("blk", "pts", None, "bond", None),
            P("blk", "pts", None, "bond", None),
            P("pts"),
        ),
        check_vma=False,
    )
```
